128 devices in a mesh: rep: 16 (over x, z), ctx: 8 (over y, core).
Axes of the slice: x: 4, y: 4, z: 4, core: 2. Of those that a mesh axis runs over, the one named last changes fastest.
Arguments:
- pre_query: bfloat16 [16, 4096, 2048], P('rep', 'ctx'), may hold values from -6 to 6
- pre_pairs: bfloat16 [16, 2, 4096, 1024], P('rep', None, 'ctx'), may hold values from -6 to 6
- prefill_len: int32 [16], P('rep'), may hold values from 2048 to 4096
- dec_query: bfloat16 [256, 2048], P('rep'), may hold values from -6 to 6
- dec_own: bfloat16 [256, 2, 1024], P('rep'), may hold values from -6 to 6
- cache: bfloat16 [256, 2, 1024, 1024], P('rep', None, 'ctx'), may hold values from -6 to 6
- cached_len: int32 [256], replicated, may hold values from 1 to 1024, as said below
- move: int32 [256], replicated, may hold values from 0 to 255, as said below
Outputs:
- pre_out: bfloat16 [16, 4096, 2048], P('rep', 'ctx')
- dec_out: bfloat16 [256, 2048], P('rep')
The draws below stay inside these ranges and needn't reach their ends.
Inputs may be any that keep to these rules, and one draw needn't show every extreme that they name: `cached_len`: some request has exactly 1024 cached positions. move is a permutation of 0 to 255; slot s lies on replica s // 16, request r has home replica r // 16, and move[r] % 16 == r % 16. The 16 requests of one replica go one to each replica, and the 16 slots of one replica serve one request of each replica.
All inputs are finite; a program needn't handle non-finite values.
Results may differ from the reference program's by a relative error of at most 0.0095.
Values may be sent and summed in bfloat16 or wider, within the bound.
No kernel may reach another device: no remote copies, remote signals or barrier semaphores. Data moves between devices by JAX's collectives and lax.ppermute only.
A program may use at most 128 MiB of HBM per device.

```python
import math
import jax
import jax.numpy as jnp
from jax import lax

QH = 16
KVH = 8
HD = 128
DEC_REP = 16
PRE = 4096
CACHE = 1024
PREFILLS = 16
REQS = 256


def prefill_pair(key):
    query_key, pair_key, place_key, sign_key = jax.random.split(jax.random.fold_in(key, 7), 4)
    query_shape = (PREFILLS, PRE, QH * HD)
    pair_shape = (PREFILLS, 2, PRE, KVH * HD)
    queries = jnp.clip(jax.random.normal(query_key, query_shape, jnp.float32), -6.0, 6.0)
    key_pairs = jnp.clip(jax.random.normal(pair_key, pair_shape, jnp.float32), -6.0, 6.0)
    aligned = 4
    places = jax.random.randint(place_key, (PREFILLS, aligned), 0, PRE // 2)
    sign_pattern = jax.random.randint(sign_key, (PREFILLS, aligned, KVH, HD), 0, 2).astype(jnp.float32) * 12.0 - 6.0
    group_size = QH // KVH
    widened = jnp.broadcast_to(sign_pattern[:, :, :, None, :], (PREFILLS, aligned, KVH, group_size, HD)).reshape(PREFILLS, aligned, QH * HD)
    row_index = jnp.arange(PREFILLS)[:, None]
    queries = queries.at[row_index, places].set(widened)
    key_pairs = key_pairs.at[row_index, 0, places].set(sign_pattern.reshape(PREFILLS, aligned, KVH * HD))
    return (queries, key_pairs)


def decode_marks(key):
    query_key, own_key, place_key, sign_key = jax.random.split(jax.random.fold_in(key, 13), 4)
    places = jax.random.permutation(place_key, REQS)[:4]
    sign_pattern = jax.random.randint(sign_key, (4, KVH, HD), 0, 2).astype(jnp.float32) * 12.0 - 6.0
    return (query_key, own_key, places, sign_pattern)


def decode_pair(key):
    query_key, own_key, places, sign_pattern = decode_marks(key)
    query_shape = (REQS, QH * HD)
    own_shape = (REQS, 2, KVH * HD)
    queries = jnp.clip(jax.random.normal(query_key, query_shape, jnp.float32), -6.0, 6.0)
    own_pairs = jnp.clip(jax.random.normal(own_key, own_shape, jnp.float32), -6.0, 6.0)
    group_size = QH // KVH
    widened = jnp.broadcast_to(sign_pattern[:, :, None, :], (4, KVH, group_size, HD)).reshape(4, QH * HD)
    queries = queries.at[places].set(widened)
    own_pairs = own_pairs.at[places[:2], 0].set(sign_pattern[:2].reshape(2, KVH * HD))
    return (queries, own_pairs)


def lengths_table(key):
    shift_key, value_key, full_key = jax.random.split(jax.random.fold_in(key, 21), 3)
    shifts = jax.random.randint(shift_key, (REQS,), 0, 4)
    raw_values = jax.random.randint(value_key, (REQS,), 0, 1 << 30)
    spans = jnp.right_shift(jnp.full((REQS,), CACHE, jnp.int32), shifts.astype(jnp.int32))
    lengths = 1 + raw_values % spans
    chosen = jax.random.randint(full_key, (), 0, REQS)
    lengths = jnp.where(jnp.arange(REQS) == chosen, CACHE, lengths)
    return lengths.astype(jnp.int32)


def move_table(key):
    first_key, second_key, offset_key = jax.random.split(jax.random.fold_in(key, 33), 3)
    replica_count = REQS // DEC_REP
    first_perm = jax.random.permutation(first_key, replica_count)
    second_perm = jax.random.permutation(second_key, replica_count)
    offsets = jax.random.permutation(offset_key, replica_count)[:DEC_REP]
    source = jnp.arange(replica_count)[:, None]
    within = jnp.arange(DEC_REP)[None, :]
    target = jnp.take(second_perm, (jnp.take(first_perm, source) + jnp.take(offsets, within)) % replica_count)
    return (target * DEC_REP + within).reshape(REQS).astype(jnp.int32)


def draw_pre_query(key, part):
    return prefill_pair(key)[0].astype(jnp.bfloat16)


def draw_pre_pairs(key, part):
    return prefill_pair(key)[1].astype(jnp.bfloat16)


def draw_dec_query(key, part):
    return decode_pair(key)[0].astype(jnp.bfloat16)


def draw_dec_own(key, part):
    return decode_pair(key)[1].astype(jnp.bfloat16)


def draw_cache(key, part):
    noise_key, spot_key = jax.random.split(jax.random.fold_in(key, 51), 2)
    shape = (REQS, 2, CACHE, KVH * HD)
    values = jnp.clip(jax.random.normal(noise_key, shape, jnp.float32), -6.0, 6.0)
    unused_query, unused_own, places, sign_pattern = decode_marks(key)
    served_by = jnp.zeros((REQS,), jnp.int32).at[move_table(key)].set(jnp.arange(REQS, dtype=jnp.int32))
    requests = jnp.take(served_by, places)
    lengths = jnp.take(lengths_table(key), requests)
    spots = jax.random.randint(spot_key, (4,), 0, 1 << 30) % lengths
    values = values.at[requests, 0, spots].set(sign_pattern.reshape(4, KVH * HD))
    return values.astype(jnp.bfloat16)


def draw_cached_len(key, part):
    return lengths_table(key)


def draw_move(key, part):
    return move_table(key)


def with_ends(drawn, key, smallest, largest):
    spot = [jax.random.randint(jax.random.fold_in(key, axis), (), 0, length) for axis, length in enumerate(drawn.shape)]
    widest = drawn.shape.index(max(drawn.shape))
    beside = spot[:widest] + [(spot[widest] + 1) % drawn.shape[widest]] + spot[widest + 1:]
    return drawn.at[tuple(spot)].set(smallest).at[tuple(beside)].set(largest)


def setup_inputs(seed: int = 0) -> dict:
    streams_of = jax.random.split(jax.random.key(seed), 9)
    pre_query = draw_pre_query(jax.random.fold_in(streams_of[8], 71), 0)
    pre_pairs = draw_pre_pairs(jax.random.fold_in(streams_of[8], 71), 0)
    prefill_len = with_ends(jax.random.randint(streams_of[2], (PREFILLS,), PRE // 2, PRE + 1), jax.random.fold_in(streams_of[2], 1), PRE // 2, PRE).astype(jnp.int32)
    dec_query = draw_dec_query(jax.random.fold_in(streams_of[8], 71), 0)
    dec_own = draw_dec_own(jax.random.fold_in(streams_of[8], 71), 0)
    cache = draw_cache(jax.random.fold_in(streams_of[8], 71), 0)
    cached_len = draw_cached_len(jax.random.fold_in(streams_of[8], 71), 0)
    move = draw_move(jax.random.fold_in(streams_of[8], 71), 0)
    return dict(pre_query=pre_query, pre_pairs=pre_pairs, prefill_len=prefill_len, dec_query=dec_query, dec_own=dec_own, cache=cache, cached_len=cached_len, move=move)


SCALE = 1.0 / 12.0
MASKED = -1e30


def prefill_one(query_rows, key_pairs, valid_len):
    group_size = QH // KVH
    query_grp = query_rows.reshape(PRE, KVH, group_size, HD)
    key_rows = key_pairs[0].reshape(PRE, KVH, HD)
    value_rows = key_pairs[1].reshape(PRE, KVH, HD)
    block_rows = math.gcd(PRE, 512)
    pieces_out = []
    for block in range(PRE // block_rows):
        upper = (block + 1) * block_rows
        query_blk = query_grp[block * block_rows:upper].astype(jnp.float32)
        key_blk = key_rows[:upper].astype(jnp.float32)
        value_blk = value_rows[:upper].astype(jnp.float32)
        scores = jnp.einsum('rgsd,kgd->gsrk', query_blk, key_blk) * SCALE
        query_pos = block * block_rows + jnp.arange(block_rows, dtype=jnp.int32)
        key_pos = jnp.arange(upper, dtype=jnp.int32)
        visible = (key_pos[None, :] <= query_pos[:, None]) & (key_pos[None, :] < valid_len)
        scores = jnp.where(visible, scores, MASKED)
        maxima = jnp.max(scores, axis=-1, keepdims=True)
        weights = jnp.where(visible, jnp.exp(scores - maxima), 0.0)
        totals = jnp.sum(weights, axis=-1)
        rounded = lax.optimization_barrier(weights.astype(jnp.bfloat16)).astype(jnp.float32)
        mixed_out = jnp.einsum('gsrk,kgd->gsrd', rounded, value_blk) / totals[..., None]
        mixed_out = jnp.transpose(mixed_out, (2, 0, 1, 3))
        mixed_out = jnp.where((query_pos < valid_len)[:, None, None, None], mixed_out, 0.0)
        pieces_out.append(mixed_out.reshape(block_rows, QH * HD))
    return jnp.concatenate(pieces_out, axis=0).astype(jnp.bfloat16)


def decode_one(query_row, key_pairs, own_pair, valid_len):
    group_size = QH // KVH
    query_grp = query_row.reshape(KVH, group_size, HD).astype(jnp.float32)
    key_rows = key_pairs[0].reshape(CACHE, KVH, HD).astype(jnp.float32)
    value_rows = key_pairs[1].reshape(CACHE, KVH, HD).astype(jnp.float32)
    own_key = own_pair[0].reshape(KVH, HD).astype(jnp.float32)
    own_value = own_pair[1].reshape(KVH, HD).astype(jnp.float32)
    scores = jnp.einsum('gsd,pgd->gsp', query_grp, key_rows) * SCALE
    visible = jnp.arange(CACHE, dtype=jnp.int32) < valid_len
    scores = jnp.where(visible, scores, MASKED)
    own_score = jnp.einsum('gsd,gd->gs', query_grp, own_key) * SCALE
    maxima = jnp.maximum(jnp.max(scores, axis=-1), own_score)
    weights = jnp.where(visible, jnp.exp(scores - maxima[..., None]), 0.0)
    own_weight = jnp.exp(own_score - maxima)
    totals = jnp.sum(weights, axis=-1) + own_weight
    rounded = lax.optimization_barrier(weights.astype(jnp.bfloat16)).astype(jnp.float32)
    mixed_out = jnp.einsum('gsp,pgd->gsd', rounded, value_rows) + own_weight[..., None] * own_value[:, None, :]
    return (mixed_out / totals[..., None]).reshape(QH * HD).astype(jnp.bfloat16)


def reference(pre_query, pre_pairs, prefill_len, dec_query, dec_own, cache, cached_len, move):
    pre_out = lax.map(lambda packed: prefill_one(packed[0], packed[1], packed[2]), (pre_query, pre_pairs, prefill_len))
    slot_query = jnp.take(dec_query, move, axis=0)
    slot_own = jnp.take(dec_own, move, axis=0)
    per_request = lax.map(lambda packed: decode_one(packed[0], packed[1], packed[2], packed[3]), (slot_query, cache, slot_own, cached_len))
    dec_out = jnp.zeros_like(dec_query).at[move].set(per_request)
    return pre_out, dec_out
```

```python
import functools
import math

import jax
import jax.numpy as jnp
from jax import lax
from jax.experimental import pallas as pl
from jax.experimental.pallas import tpu as pltpu
from jax.sharding import PartitionSpec as P

QH = 16
KVH = 8
HD = 128
SCALE = 1.0 / 12.0
EXP2_SCALE = SCALE * math.log2(math.e)
MASKED = -1e30
TILE = 256
CHUNK = 1024
BF16 = jnp.bfloat16
F32 = jnp.float32


def swap(array, flip):
    return lax.ppermute(array, "ctx", [(i, i ^ flip) for i in range(8)])


def lanes(array, at, width):
    return lax.dynamic_slice_in_dim(array, at * width, width, axis=array.ndim - 1)


def attend_kernel(table, *refs, key_pieces, value_pieces, query_pieces, count_in):
    inputs = refs[:count_in]
    out_ref = refs[count_in]
    keys, values, queries, acc, top, sems = refs[count_in + 1 :]
    me = table[0]
    valid = table[1]
    core = me & 1
    copies = []

    def view(piece):
        which, index, kind = piece
        ref = inputs[which]
        if index is not None:
            ref = ref.at[index]
        if kind == "own":
            ref = ref.at[:, pl.ds(pl.multiple_of(me * HD, HD), HD)]
        elif kind == "core":
            ref = ref.at[:, pl.ds(pl.multiple_of(core * HD, HD), HD)]
        elif kind == "query":
            ref = ref.at[:, pl.ds(pl.multiple_of(me * 2 * HD, 2 * HD), 2 * HD)]
        return ref

    def put(piece, dest):
        copy = pltpu.make_async_copy(view(piece), dest, sems.at[len(copies)])
        copy.start()
        copies.append(copy)

    for z, piece in enumerate(key_pieces):
        at = pl.multiple_of((me ^ z) * 512, 512)
        put(piece, keys.at[pl.ds(at, 512)])
    for z, piece in enumerate(value_pieces):
        at = pl.multiple_of((me ^ z) * 512, 512)
        put(piece, values.at[pl.ds(at, 512), 0:HD])
    for n, piece in enumerate(query_pieces):
        put(piece, queries.at[n])
    values[:, HD:] = jnp.ones((values.shape[0], HD), BF16)
    for copy in copies:
        copy.wait()

    tiles = 512 // TILE

    def one_tile(step, unused):
        n = step // tiles
        part = step % tiles
        first = table[2 + n] * 512 + part * TILE
        rows = pl.ds(pl.multiple_of(part * TILE, TILE), TILE)

        @pl.when(first >= valid)
        def _():
            out_ref[n, rows, :] = jnp.zeros((TILE, 2 * HD), BF16)

        @pl.when(first < valid)
        def _():
            rest = first % CHUNK
            base = pl.multiple_of(first - rest, CHUNK)

            for width in range(TILE, CHUNK + 1, TILE):

                @pl.when(rest == width - TILE)
                def _(width=width):
                    key = keys[pl.ds(base, width)]
                    value = values[pl.ds(base, width)]
                    seen = lax.broadcasted_iota(
                        jnp.int32, (TILE, width), 1
                    ) <= lax.broadcasted_iota(jnp.int32, (TILE, width), 0) + (width - TILE)
                    for g in range(2):
                        query = queries[n, rows, g * HD : (g + 1) * HD]
                        score = lax.dot_general(
                            query, key, (((1,), (1,)), ((), ())), preferred_element_type=F32
                        )
                        score = jnp.where(seen, score, MASKED)
                        new_top = jnp.max(score, axis=1, keepdims=True)
                        top[g] = jnp.broadcast_to(new_top, (TILE, HD))
                        weight = jnp.exp2((score - new_top) * EXP2_SCALE).astype(BF16)
                        acc[g] = jnp.dot(weight, value, preferred_element_type=F32)

            def full(c, unused):
                at = pl.multiple_of(c * CHUNK, CHUNK)
                key = keys[pl.ds(at, CHUNK)]
                value = values[pl.ds(at, CHUNK)]
                for g in range(2):
                    query = queries[n, rows, g * HD : (g + 1) * HD]
                    score = lax.dot_general(
                        query, key, (((1,), (1,)), ((), ())), preferred_element_type=F32
                    )
                    old_top = top[g]
                    new_top = jnp.maximum(old_top, jnp.max(score, axis=1, keepdims=True))
                    factor = jnp.exp2((old_top - new_top) * EXP2_SCALE)
                    top[g] = new_top
                    weight = jnp.exp2((score - new_top[:, :1]) * EXP2_SCALE).astype(BF16)
                    more = jnp.dot(weight, value, preferred_element_type=F32)
                    acc[g, :, :HD] = acc[g, :, :HD] * factor + more[:, :HD]
                    acc[g, :, HD:] = acc[g, :, HD:] * factor + more[:, HD:]
                return unused

            lax.fori_loop(0, first // CHUNK, full, 0)
            live = lax.broadcasted_iota(jnp.int32, (TILE, HD), 0) + first < valid
            for g in range(2):
                mixed = acc[g, :, :HD] / acc[g, :, HD:]
                out_ref[n, rows, g * HD : (g + 1) * HD] = jnp.where(live, mixed, 0.0).astype(BF16)

        return unused

    lax.fori_loop(0, len(query_pieces) * tiles, one_tile, 0)


def attend(table, arrays, key_pieces, value_pieces, query_pieces, name):
    n = len(query_pieces)
    kernel = functools.partial(
        attend_kernel,
        key_pieces=key_pieces,
        value_pieces=value_pieces,
        query_pieces=query_pieces,
        count_in=len(arrays),
    )
    return pl.pallas_call(
        kernel,
        grid_spec=pltpu.PrefetchScalarGridSpec(
            num_scalar_prefetch=1,
            grid=(1,),
            in_specs=[pl.BlockSpec(memory_space=pl.ANY)] * len(arrays),
            out_specs=pl.BlockSpec((n, 512, 2 * HD), lambda i, t: (0, 0, 0)),
            scratch_shapes=[
                pltpu.VMEM((4096, HD), BF16),
                pltpu.VMEM((4096, 2 * HD), BF16),
                pltpu.VMEM((n, 512, 2 * HD), BF16),
                pltpu.VMEM((2, TILE, 2 * HD), F32),
                pltpu.VMEM((2, TILE, HD), F32),
                pltpu.SemaphoreType.DMA((16 + n,)),
            ],
        ),
        out_shape=jax.ShapeDtypeStruct((n, 512, 2 * HD), BF16),
        compiler_params=pltpu.CompilerParams(vmem_limit_bytes=40 * 2**20),
        cost_estimate=pl.CostEstimate(
            flops=n * 1_200_000_000, bytes_accessed=4_000_000, transcendentals=n * 2_000_000
        ),
        name=name,
    )(table, *arrays)


def join_kernel(table, *refs, pieces, count_in):
    inputs = refs[:count_in]
    out_ref, sems = refs[count_in:]
    me = table[0]
    copies = []
    for z, (which, index) in enumerate(pieces):
        at = pl.multiple_of((me ^ z) * 2 * HD, 2 * HD)
        copy = pltpu.make_async_copy(
            inputs[which].at[index], out_ref.at[0, :, pl.ds(at, 2 * HD)], sems.at[z]
        )
        copy.start()
        copies.append(copy)
    for copy in copies:
        copy.wait()


def join(table, arrays, pieces):
    return pl.pallas_call(
        functools.partial(join_kernel, pieces=pieces, count_in=len(arrays)),
        grid_spec=pltpu.PrefetchScalarGridSpec(
            num_scalar_prefetch=1,
            grid=(1,),
            in_specs=[pl.BlockSpec(memory_space=pl.ANY)] * len(arrays),
            out_specs=pl.BlockSpec((1, 512, QH * HD), lambda i, t: (0, 0, 0)),
            scratch_shapes=[pltpu.SemaphoreType.DMA((8,))],
        ),
        out_shape=jax.ShapeDtypeStruct((1, 512, QH * HD), BF16),
        compiler_params=pltpu.CompilerParams(vmem_limit_bytes=16 * 2**20),
        cost_estimate=pl.CostEstimate(
            flops=10_000_000, bytes_accessed=4_000_000, transcendentals=0
        ),
        name="join",
    )(table, *arrays)


def prefill(me, pre_query, pre_pairs, valid_len):
    core = me & 1
    chip = me >> 1
    key, value = pre_pairs[0, 0], pre_pairs[0, 1]
    query = pre_query[0]

    def to_chip(array, x):
        return lanes(array, chip ^ x, 2 * HD)

    key_1 = swap(jnp.stack([to_chip(key, 1), to_chip(key, 2)]), 2)
    value_1 = swap(jnp.stack([to_chip(value, 3), to_chip(value, 2)]), 6)
    query_by = query.reshape(512, 4, 2, 2 * HD)
    across = lax.dynamic_index_in_dim(query_by, 1 - core, 2, keepdims=False)

    def pick(array, x):
        return lax.dynamic_index_in_dim(array, chip ^ x, 1, keepdims=False)

    query_x = swap(jnp.stack([pick(across, x) for x in range(4)]), 1)
    key_2 = swap(jnp.stack([to_chip(key, 3), key_1[1]]), 6)
    value_2 = swap(jnp.stack([to_chip(value, 1), value_1[1]]), 2)

    def mine(x):
        return lanes(query, ((chip ^ x) << 1) | core, 2 * HD)

    query_a1 = swap(jnp.stack([mine(1), mine(2)]), 2)
    query_b1 = swap(jnp.stack([query_x[3], query_x[2]]), 6)

    def other(array):
        return lanes(array, 1 - core, HD)

    pairs_x = swap(
        jnp.stack(
            [
                lanes(key, me ^ 1, HD),
                other(key_1[0]),
                other(key_2[1]),
                other(key_2[0]),
                lanes(value, me ^ 1, HD),
                other(value_2[0]),
                other(value_2[1]),
                other(value_1[0]),
            ]
        ),
        1,
    )
    query_a2 = swap(jnp.stack([mine(3), query_a1[1]]), 6)
    query_b2 = swap(jnp.stack([query_x[1], query_b1[1]]), 2)

    arrays = [
        pre_pairs[0],
        key_1,
        key_2,
        value_1,
        value_2,
        pairs_x,
        query,
        query_a1,
        query_a2,
        query_b1,
        query_b2,
        query_x,
    ]
    key_pieces = [
        (0, 0, "own"),
        (5, 0, None),
        (1, 0, "core"),
        (5, 1, None),
        (2, 1, "core"),
        (5, 2, None),
        (2, 0, "core"),
        (5, 3, None),
    ]
    value_pieces = [
        (0, 1, "own"),
        (5, 4, None),
        (4, 0, "core"),
        (5, 5, None),
        (4, 1, "core"),
        (5, 6, None),
        (3, 0, "core"),
        (5, 7, None),
    ]
    query_pieces = {
        0: (6, None, "query"),
        1: (11, 0, None),
        2: (7, 0, None),
        3: (10, 0, None),
        4: (8, 1, None),
        5: (10, 1, None),
        6: (8, 0, None),
        7: (9, 0, None),
    }
    order = [6, 4, 3, 5, 2, 7, 0, 1]
    table = jnp.stack([me, valid_len] + [me ^ z for z in order]).astype(jnp.int32)
    mixed = attend(
        table, arrays, key_pieces, value_pieces, [query_pieces[z] for z in order], "attend"
    )
    out = {z: mixed[i] for i, z in enumerate(order)}
    back_a1 = swap(jnp.stack([out[6], out[4]]), 6)
    back_b1 = swap(jnp.stack([out[3], out[5]]), 2)
    back_a2 = swap(jnp.stack([out[2], back_a1[1]]), 2)
    back_b2 = swap(jnp.stack([out[7], back_b1[1]]), 6)
    back_x = swap(jnp.stack([out[1], back_b1[0], back_b2[1], back_b2[0]]), 1)
    return join(
        table,
        [mixed, back_a1, back_a2, back_x],
        [(0, 6), (3, 0), (2, 0), (3, 1), (2, 1), (3, 2), (1, 0), (3, 3)],
    )


def cache_kernel(table, query_ref, cache_ref, out_ref):
    n = pl.program_id(0)
    span_base = table[0]
    length = table[1 + n]
    span = cache_ref.shape[2]
    query = query_ref[0]
    head = lax.broadcasted_iota(jnp.int32, (QH, KVH * HD), 0) // 2
    block = lax.broadcasted_iota(jnp.int32, (QH, KVH * HD), 1) // HD
    wide = jnp.where(head == block, jnp.concatenate([query] * KVH, axis=1), 0).astype(BF16)
    key = cache_ref[0, 0]
    value = cache_ref[0, 1]
    score = (
        lax.dot_general(wide, key, (((1,), (1,)), ((), ())), preferred_element_type=F32) * SCALE
    )
    visible = lax.broadcasted_iota(jnp.int32, (QH, span), 1) + span_base < length
    score = jnp.where(visible, score, MASKED)
    top = jnp.max(score, axis=1, keepdims=True).astype(BF16)
    weight = jnp.where(visible, jnp.exp(score - top.astype(F32)), 0.0)
    total = jnp.sum(weight, axis=1, keepdims=True)
    mixed = jnp.dot(weight.astype(BF16), value, preferred_element_type=F32)
    mixed = jnp.where(head == block, mixed, 0.0)
    picked = mixed[:, :HD]
    for h in range(1, KVH):
        picked = picked + mixed[:, h * HD : (h + 1) * HD]
    out_ref[0, :, :HD] = picked.astype(BF16)
    lane = lax.broadcasted_iota(jnp.int32, (QH, HD), 1)
    out_ref[0, :, HD:] = jnp.where(
        lane == 0, jnp.broadcast_to(top.astype(F32), (QH, HD)), jnp.broadcast_to(total, (QH, HD))
    ).astype(BF16)


def over_cache(span_base, lengths, dest_rep, queries, cache):
    count = cache.shape[0]
    span = cache.shape[2]
    table = jnp.concatenate([jnp.stack([span_base]), lengths, dest_rep]).astype(jnp.int32)
    return pl.pallas_call(
        cache_kernel,
        grid_spec=pltpu.PrefetchScalarGridSpec(
            num_scalar_prefetch=1,
            grid=(count,),
            in_specs=[
                pl.BlockSpec((1, QH, HD), lambda n, t: (t[1 + count + n], 0, 0)),
                pl.BlockSpec((1, 2, span, KVH * HD), lambda n, t: (n, 0, 0, 0)),
            ],
            out_specs=pl.BlockSpec((1, QH, 2 * HD), lambda n, t: (t[1 + count + n], 0, 0)),
        ),
        out_shape=jax.ShapeDtypeStruct((count, QH, 2 * HD), BF16),
        compiler_params=pltpu.CompilerParams(vmem_limit_bytes=16 * 2**20),
        cost_estimate=pl.CostEstimate(
            flops=1_000_000_000, bytes_accessed=8_500_000, transcendentals=300_000
        ),
        name="over_cache",
    )(table, queries, cache)


def merge(left, right):
    left, right = left.astype(F32), right.astype(F32)
    left_top, right_top = left[..., HD : HD + 1], right[..., HD : HD + 1]
    new_top = jnp.maximum(left_top, right_top)
    left_factor = jnp.exp(left_top - new_top)
    right_factor = jnp.exp(right_top - new_top)
    weighted = left[..., :HD] * left_factor + right[..., :HD] * right_factor
    total = left[..., HD + 1 : HD + 2] * left_factor + right[..., HD + 1 : HD + 2] * right_factor
    return weighted, new_top, total


def packed(weighted, top, total):
    return jnp.concatenate([weighted, top, total], axis=-1).astype(BF16)


def decode(me, dec_query, dec_own, cache, cached_len, move):
    per_rep = cache.shape[0]
    span = cache.shape[2]
    rep = lax.axis_index("rep")
    reps = lax.axis_size("rep")
    requests = move.shape[0]
    ids = jnp.arange(per_rep, dtype=jnp.int32)
    dest_rep = lax.dynamic_slice_in_dim(move, rep * per_rep, per_rep) // per_rep
    lengths = lax.dynamic_slice_in_dim(cached_len, rep * per_rep, per_rep)
    my_slots = rep * per_rep + ids
    served = jnp.sum(
        jnp.where(
            move[None, :] == my_slots[:, None], jnp.arange(requests, dtype=jnp.int32)[None, :], 0
        ),
        axis=1,
    )
    source_rep = served // per_rep
    to_home = jnp.arange(reps, dtype=jnp.int32)[:, None] == source_rep[None, :]
    outgoing = jnp.dot(to_home.astype(BF16), dec_query, preferred_element_type=F32).astype(BF16)
    arrived = lax.all_to_all(outgoing, "rep", split_axis=0, concat_axis=0, tiled=True)
    partial = over_cache(me * span, lengths, dest_rep, arrived.reshape(reps, QH, HD), cache)
    partial = partial[:, :, : HD + 2].reshape(reps, QH * (HD + 2))
    back = lax.all_to_all(partial, "rep", split_axis=0, concat_axis=0, tiled=True)
    back = jnp.dot(
        (source_rep[:, None] == jnp.arange(reps, dtype=jnp.int32)[None, :]).astype(BF16),
        back,
        preferred_element_type=F32,
    ).astype(BF16)
    back = back.reshape(per_rep, QH, HD + 2)
    back = packed(*merge(back, swap(back, 1)))
    back = packed(*merge(back, swap(back, 2)))
    weighted, top, total = merge(back, swap(back, 6))
    query_heads = dec_query.reshape(per_rep, KVH, 2, HD)
    own_key = dec_own[:, 0].reshape(per_rep, KVH, HD)
    own_value = dec_own[:, 1].reshape(per_rep, KVH, HD).astype(F32)
    own_score = (
        jnp.sum(query_heads.astype(F32) * own_key[:, :, None, :].astype(F32), axis=-1) * SCALE
    ).reshape(per_rep, QH, 1)
    own_value = jnp.broadcast_to(own_value[:, :, None, :], (per_rep, KVH, 2, HD)).reshape(
        per_rep, QH, HD
    )
    new_top = jnp.maximum(top, own_score)
    keep = jnp.exp(top - new_top)
    own_weight = jnp.exp(own_score - new_top)
    mixed = (weighted * keep + own_weight * own_value) / (total * keep + own_weight)
    return mixed.reshape(per_rep, QH * HD).astype(BF16)


def on_device(pre_query, pre_pairs, prefill_len, dec_query, dec_own, cache, cached_len, move):
    me = lax.axis_index("ctx").astype(jnp.int32)
    dec_out = decode(me, dec_query, dec_own, cache, cached_len, move)
    pre_out = prefill(me, pre_query, pre_pairs, prefill_len[0])
    return (pre_out, dec_out)


def solution(mesh):
    in_specs = (
        P("rep", "ctx", None),
        P("rep", None, "ctx", None),
        P("rep"),
        P("rep", None),
        P("rep", None, None),
        P("rep", None, "ctx", None),
        P(),
        P(),
    )
    out_specs = (P("rep", "ctx", None), P("rep", None))
    return jax.shard_map(
        on_device, mesh=mesh, in_specs=in_specs, out_specs=out_specs, check_vma=False
    )
```

```python
import functools
import math

import jax
import jax.numpy as jnp
from jax import lax
from jax.experimental import pallas as pl
from jax.experimental.pallas import tpu as pltpu
from jax.sharding import PartitionSpec as P


QH = 16
KVH = 8
HD = 128
SCALE = 1.0 / 12.0
EXP2_SCALE = SCALE * math.log2(math.e)
MASKED = -1e30
TILE = 128
CHUNK = 1024
VMEM = 63_000_000
SMALL = 20_000_000
BF16 = jnp.bfloat16
F32 = jnp.float32


def swap(array, flip):
    return lax.ppermute(array, "ctx", [(i, i ^ flip) for i in range(8)])


def exchange(array):
    return lax.all_to_all(array, "rep", split_axis=0, concat_axis=0, tiled=True)


def lanes(array, at, width):
    return lax.dynamic_slice_in_dim(array, at * width, width, axis=array.ndim - 1)


def attend_kernel(table, *refs, key_pieces, value_pieces, query_pieces, blocks, out_sizes, count_in):
    inputs = refs[:count_in]
    out_refs = refs[count_in : count_in + len(out_sizes)]
    token = refs[count_in + len(out_sizes)]
    keys, values, queries, mixes, acc, top, sems, out_sems = refs[count_in + len(out_sizes) + 1 :]
    me = table[0]
    valid = table[1]
    core = me & 1
    copies = []

    def view(piece):
        which, index, kind = piece
        ref = inputs[which]
        if index is not None:
            ref = ref.at[index]
        if kind == "own":
            ref = ref.at[:, pl.ds(pl.multiple_of(me * HD, HD), HD)]
        elif kind == "core":
            ref = ref.at[:, pl.ds(pl.multiple_of(core * HD, HD), HD)]
        elif kind == "query":
            ref = ref.at[:, pl.ds(pl.multiple_of(me * 2 * HD, 2 * HD), 2 * HD)]
        return ref

    def put(piece, dest):
        copy = pltpu.make_async_copy(view(piece), dest, sems.at[len(copies)])
        copy.start()
        copies.append(copy)

    for z, piece in enumerate(key_pieces):
        at = pl.multiple_of((me ^ z) * 512, 512)
        put(piece, keys.at[pl.ds(at, 512)])
    for z, piece in enumerate(value_pieces):
        at = pl.multiple_of((me ^ z) * 512, 512)
        put(piece, values.at[pl.ds(at, 512), 0:HD])
    for n, piece in enumerate(query_pieces):
        put(piece, queries.at[n])
    values[:, HD:] = jnp.ones((values.shape[0], HD), BF16)
    for copy in copies:
        copy.wait()

    halves = 1
    parts = [(t, slice(t * TILE, (t + 1) * TILE)) for t in range(512 // TILE)]

    def one_block(n, block):
        first = block * 512

        @pl.when(first >= valid)
        def _():
            mixes[n] = jnp.zeros((512, 2 * HD), BF16)

        @pl.when(first < valid)
        def _():
            rest = first % CHUNK
            base = pl.multiple_of(first - rest, CHUNK)

            for start in range(0, CHUNK, 512):

                @pl.when(rest == start)
                def _(start=start):
                    for t, rows in parts:
                        width = start + (t + 1) * TILE
                        key = keys[pl.ds(base, width)]
                        value = values[pl.ds(base, width)]
                        seen = lax.broadcasted_iota(
                            jnp.int32, (TILE, width), 1
                        ) <= lax.broadcasted_iota(jnp.int32, (TILE, width), 0) + (width - TILE)
                        for g in range(2):
                            query = queries[n, rows, g * HD : (g + 1) * HD]
                            score = lax.dot_general(
                                query, key, (((1,), (1,)), ((), ())), preferred_element_type=F32
                            )
                            score = jnp.where(seen, score, MASKED)
                            new_top = jnp.max(score, axis=1, keepdims=True)
                            top[g, rows] = jnp.broadcast_to(new_top, (TILE, HD))
                            weight = jnp.exp2((score - new_top) * EXP2_SCALE).astype(BF16)
                            acc[g, rows] = jnp.dot(weight, value, preferred_element_type=F32)

            def full(step, unused):
                at = pl.multiple_of((step // halves) * CHUNK, CHUNK)
                half = (step % halves) * (512 // halves)
                key = keys[pl.ds(at, CHUNK)]
                value = values[pl.ds(at, CHUNK)]
                for t in range(512 // TILE // halves):
                    rows = pl.ds(pl.multiple_of(half + t * TILE, TILE), TILE)
                    for g in range(2):
                        query = queries[n, rows, g * HD : (g + 1) * HD]
                        score = lax.dot_general(
                            query, key, (((1,), (1,)), ((), ())), preferred_element_type=F32
                        )
                        old_top = top[g, rows]
                        new_top = jnp.maximum(old_top, jnp.max(score, axis=1, keepdims=True))
                        factor = jnp.exp2((old_top - new_top) * EXP2_SCALE)
                        top[g, rows] = new_top
                        weight = jnp.exp2((score - new_top[:, :1]) * EXP2_SCALE).astype(BF16)
                        more = jnp.dot(weight, value, preferred_element_type=F32)
                        acc[g, rows, :HD] = acc[g, rows, :HD] * factor + more[:, :HD]
                        acc[g, rows, HD:] = acc[g, rows, HD:] * factor + more[:, HD:]
                return unused

            lax.fori_loop(0, (first // CHUNK) * halves, full, 0)
            live = lax.broadcasted_iota(jnp.int32, (512, HD), 0) + first < valid
            for g in range(2):
                mixed = acc[g, :, :HD] / acc[g, :, HD:]
                mixes[n, :, g * HD : (g + 1) * HD] = jnp.where(live, mixed, 0.0).astype(BF16)

    leaving = []
    for out_ref, size in zip(out_refs, out_sizes):
        for i in range(size):
            n = len(leaving)
            leaving.append(
                pltpu.make_async_copy(mixes.at[n], out_ref.at[i], out_sems.at[n])
            )

    def step(n, unused):
        flip = jnp.int32(blocks[0])
        for more in range(1, len(blocks)):
            flip = jnp.where(n == more, blocks[more], flip)
        one_block(n, me ^ flip)
        return unused

    lax.fori_loop(0, len(blocks), step, 0)
    for copy in leaving:
        copy.start()
    for copy in leaving:
        copy.wait()
    token[...] = jnp.zeros_like(token)


def attend_call(table, arrays, key_pieces, value_pieces, query_pieces, blocks, out_sizes):
    n = len(query_pieces)
    kernel = functools.partial(
        attend_kernel,
        key_pieces=key_pieces,
        value_pieces=value_pieces,
        query_pieces=query_pieces,
        blocks=blocks,
        out_sizes=out_sizes,
        count_in=len(arrays),
    )
    return pl.pallas_call(
        kernel,
        grid_spec=pltpu.PrefetchScalarGridSpec(
            num_scalar_prefetch=1,
            grid=(1,),
            in_specs=[pl.BlockSpec(memory_space=pl.ANY)] * len(arrays),
            out_specs=[pl.BlockSpec(memory_space=pl.ANY)] * len(out_sizes)
            + [pl.BlockSpec((8, HD), lambda i, t: (0, 0))],
            scratch_shapes=[
                pltpu.VMEM((4096, HD), BF16),
                pltpu.VMEM((4096, 2 * HD), BF16),
                pltpu.VMEM((n, 512, 2 * HD), BF16),
                pltpu.VMEM((n, 512, 2 * HD), BF16),
                pltpu.VMEM((2, 512, 2 * HD), F32),
                pltpu.VMEM((2, 512, HD), F32),
                pltpu.SemaphoreType.DMA((16 + n,)),
                pltpu.SemaphoreType.DMA((n,)),
            ],
        ),
        out_shape=[jax.ShapeDtypeStruct((size, 512, 2 * HD), BF16) for size in out_sizes]
        + [jax.ShapeDtypeStruct((8, HD), F32)],
        compiler_params=pltpu.CompilerParams(vmem_limit_bytes=SMALL),
        cost_estimate=pl.CostEstimate(
            flops=n * 1_200_000_000, bytes_accessed=4_000_000, transcendentals=n * 2_000_000
        ),
    )(table, *arrays)


def collect_kernel(table, *refs, outs, count_in):
    inputs = refs[:count_in]
    out_refs = refs[count_in:-1]
    sems = refs[-1]
    me = table[0]
    copies = []
    for out_ref, pieces in zip(out_refs, outs):
        for n, (which, index, lane, out_lane, width) in enumerate(pieces):
            ref = inputs[which]
            if index is not None:
                ref = ref.at[index]
            if lane is not None:
                ref = ref.at[:, pl.ds(pl.multiple_of(lane(me) * width, width), width)]
            if out_lane is None:
                dest = out_ref.at[n]
            else:
                at = pl.multiple_of(out_lane(me) * width, width)
                dest = out_ref.at[0, :, pl.ds(at, width)]
            copy = pltpu.make_async_copy(ref, dest, sems.at[len(copies)])
            copy.start()
            copies.append(copy)
    for copy in copies:
        copy.wait()


def collect(table, arrays, outs):
    shapes = []
    for pieces in outs:
        if pieces[0][3] is None:
            shapes.append((len(pieces), 512, pieces[0][4]))
        else:
            shapes.append((1, 512, len(pieces) * pieces[0][4]))
    total = sum(math.prod(shape) for shape in shapes)
    result = pl.pallas_call(
        functools.partial(collect_kernel, outs=outs, count_in=len(arrays)),
        grid_spec=pltpu.PrefetchScalarGridSpec(
            num_scalar_prefetch=1,
            grid=(1,),
            in_specs=[pl.BlockSpec(memory_space=pl.ANY)] * len(arrays),
            out_specs=[pl.BlockSpec(shape, lambda i, t: (0, 0, 0)) for shape in shapes],
            scratch_shapes=[pltpu.SemaphoreType.DMA((sum(len(p) for p in outs),))],
        ),
        out_shape=[jax.ShapeDtypeStruct(shape, BF16) for shape in shapes],
        compiler_params=pltpu.CompilerParams(vmem_limit_bytes=SMALL),
        cost_estimate=pl.CostEstimate(
            flops=total * 2, bytes_accessed=total * 4, transcendentals=0
        ),
    )(table, *arrays)
    return result


def after(value, *others):
    return lax.optimization_barrier((value, *others))[0]


def wide(array, at):
    return lanes(array, at, 2 * HD)


def prefill_pairs(me, pre_pairs):
    chip = me >> 1
    key, value = pre_pairs[0, 0], pre_pairs[0, 1]
    key_1 = jnp.stack([wide(key, chip ^ 1), wide(key, chip ^ 2)])
    value_1 = jnp.stack([wide(value, chip ^ 3), wide(value, chip ^ 2)])
    return key_1, value_1


def prefill_pairs_on(me, pre_pairs, key_1, value_1):
    chip = me >> 1
    key, value = pre_pairs[0, 0], pre_pairs[0, 1]
    key_2 = jnp.stack([wide(key, chip ^ 3), key_1[1]])
    value_2 = jnp.stack([wide(value, chip ^ 1), value_1[1]])
    return key_2, value_2


def prefill_queries(me, query):
    query_x = swap(jnp.stack([wide(query, me ^ 7), wide(query, me ^ 5)]), 1)
    query_y = swap(jnp.stack([wide(query, me ^ 1), wide(query, me ^ 3)]), 1)
    query_a1 = jnp.stack([wide(query, me ^ 2), wide(query, me ^ 4)])
    return query_x, query_y, query_a1


def prefill_across(table, pairs, key_1, key_2, value_1, value_2):
    def other(which, index):
        return (which, index, lambda m: 1 - (m & 1), None, HD)

    def own(index):
        return (0, index, lambda m: m ^ 1, None, HD)

    (pairs_x,) = collect(
        table,
        [pairs, key_1, key_2, value_1, value_2],
        [
            [
                own(0),
                other(1, 0),
                other(2, 1),
                other(2, 0),
                own(1),
                other(4, 0),
                other(4, 1),
                other(3, 0),
            ]
        ],
    )
    return swap(pairs_x, 1)


KEY_PIECES = [
    (0, 0, "own"),
    (5, 0, None),
    (1, 0, "core"),
    (5, 1, None),
    (2, 1, "core"),
    (5, 2, None),
    (2, 0, "core"),
    (5, 3, None),
]
VALUE_PIECES = [
    (0, 1, "own"),
    (5, 4, None),
    (4, 0, "core"),
    (5, 5, None),
    (4, 1, "core"),
    (5, 6, None),
    (3, 0, "core"),
    (5, 7, None),
]


def part(table, keyed, arrays, pieces, blocks, out_sizes):
    return attend_call(table, keyed + arrays, KEY_PIECES, VALUE_PIECES, pieces, blocks, out_sizes)


def prefill_join(table, outs):
    def place(which, index, z):
        return (which, index, None, lambda m: m ^ z, 2 * HD)

    places = [(0, 0), (4, 0), (1, 1), (4, 1), (3, 0), (4, 3), (2, 0), (4, 2)]
    (joined,) = collect(
        table, outs, [[place(which, index, z) for z, (which, index) in enumerate(places)]]
    )
    return joined


def cache_kernel(table, query_ref, cache_ref, out_ref):
    span_base = table[0]
    count = query_ref.shape[0]
    step_count, span = cache_ref.shape[0], cache_ref.shape[2]
    head = lax.broadcasted_iota(jnp.int32, (QH, KVH * HD), 0) // 2
    block = lax.broadcasted_iota(jnp.int32, (QH, KVH * HD), 1) // HD
    lane = lax.broadcasted_iota(jnp.int32, (QH, HD), 1)
    position = lax.broadcasted_iota(jnp.int32, (QH, span), 1) + span_base
    rows, scores, seen = [], [], []
    for i in range(step_count):
        n = pl.program_id(0) * step_count + i
        rows.append(table[1 + count + n])
        query = query_ref[rows[i]]
        wide = jnp.where(head == block, jnp.concatenate([query] * KVH, axis=1), 0).astype(BF16)
        scores.append(
            lax.dot_general(
                wide, cache_ref[i, 0], (((1,), (1,)), ((), ())), preferred_element_type=F32
            )
        )
        seen.append(position < table[1 + n])
    visible = jnp.concatenate(seen, axis=0)
    score = jnp.where(visible, jnp.concatenate(scores, axis=0) * SCALE, MASKED)
    top = jnp.max(score, axis=1, keepdims=True).astype(BF16).astype(F32)
    weight = jnp.where(visible, jnp.exp(score - top), 0.0)
    total = jnp.sum(weight, axis=1, keepdims=True)
    weight = weight.astype(BF16)
    for i in range(step_count):
        part = slice(i * QH, (i + 1) * QH)
        mixed = jnp.dot(weight[part], cache_ref[i, 1], preferred_element_type=F32)
        mixed = jnp.where(head == block, mixed, 0.0)
        picked = mixed[:, :HD]
        for h in range(1, KVH):
            picked = picked + mixed[:, h * HD : (h + 1) * HD]
        out_ref[rows[i], :, :HD] = picked.astype(BF16)
        out_ref[rows[i], :, HD:] = jnp.where(
            lane == 0,
            jnp.broadcast_to(top[part], (QH, HD)),
            jnp.broadcast_to(total[part], (QH, HD)),
        ).astype(BF16)


def over_cache(span_base, lengths, dest_rep, queries, cache):
    count = cache.shape[0]
    span = cache.shape[2]
    each = math.gcd(count, 4)
    table = jnp.concatenate([jnp.stack([span_base]), lengths, dest_rep]).astype(jnp.int32)
    return pl.pallas_call(
        cache_kernel,
        grid_spec=pltpu.PrefetchScalarGridSpec(
            num_scalar_prefetch=1,
            grid=(count // each,),
            in_specs=[
                pl.BlockSpec((count, QH, HD), lambda n, t: (0, 0, 0)),
                pl.BlockSpec((each, 2, span, KVH * HD), lambda n, t: (n, 0, 0, 0)),
            ],
            out_specs=pl.BlockSpec((count, QH, 2 * HD), lambda n, t: (0, 0, 0)),
        ),
        out_shape=jax.ShapeDtypeStruct((count, QH, 2 * HD), BF16),
        compiler_params=pltpu.CompilerParams(vmem_limit_bytes=VMEM),
        cost_estimate=pl.CostEstimate(
            flops=8_000_000_000, bytes_accessed=8_500_000, transcendentals=300_000
        ),
        name="over_cache",
    )(table, queries, cache)


def merge(left, right):
    left, right = left.astype(F32), right.astype(F32)
    left_top, right_top = left[..., HD : HD + 1], right[..., HD : HD + 1]
    new_top = jnp.maximum(left_top, right_top)
    left_factor = jnp.exp(left_top - new_top)
    right_factor = jnp.exp(right_top - new_top)
    weighted = left[..., :HD] * left_factor + right[..., :HD] * right_factor
    total = left[..., HD + 1 : HD + 2] * left_factor + right[..., HD + 1 : HD + 2] * right_factor
    return weighted, new_top, total


def packed(weighted, top, total):
    return jnp.concatenate([weighted, top, total], axis=-1).astype(BF16)


def decode_tables(cache, cached_len, move):
    per_rep = cache.shape[0]
    rep = lax.axis_index("rep")
    requests = move.shape[0]
    ids = jnp.arange(per_rep, dtype=jnp.int32)
    dest_rep = lax.dynamic_slice_in_dim(move, rep * per_rep, per_rep) // per_rep
    lengths = lax.dynamic_slice_in_dim(cached_len, rep * per_rep, per_rep)
    my_slots = rep * per_rep + ids
    served = jnp.sum(
        jnp.where(
            move[None, :] == my_slots[:, None], jnp.arange(requests, dtype=jnp.int32)[None, :], 0
        ),
        axis=1,
    )
    return dest_rep, lengths, served // per_rep


def decode_send(source_rep, dec_query):
    reps = lax.axis_size("rep")
    to_home = jnp.arange(reps, dtype=jnp.int32)[:, None] == source_rep[None, :]
    return jnp.dot(to_home.astype(BF16), dec_query, preferred_element_type=F32).astype(BF16)


def decode_home(me, lengths, dest_rep, arrived, cache):
    reps = lax.axis_size("rep")
    span = cache.shape[2]
    partial = over_cache(me * span, lengths, dest_rep, arrived.reshape(reps, QH, HD), cache)
    return partial[:, :, : HD + 2].reshape(reps, QH * (HD + 2))


def decode_order(source_rep, back):
    reps = back.shape[0]
    back = jnp.dot(
        (source_rep[:, None] == jnp.arange(reps, dtype=jnp.int32)[None, :]).astype(BF16),
        back,
        preferred_element_type=F32,
    ).astype(BF16)
    return back.reshape(source_rep.shape[0], QH, HD + 2)


def decode_finish(weighted, top, total, dec_query, dec_own):
    per_rep = dec_query.shape[0]
    query_heads = dec_query.reshape(per_rep, KVH, 2, HD)
    own_key = dec_own[:, 0].reshape(per_rep, KVH, HD)
    own_value = dec_own[:, 1].reshape(per_rep, KVH, HD).astype(F32)
    own_score = (
        jnp.sum(query_heads.astype(F32) * own_key[:, :, None, :].astype(F32), axis=-1) * SCALE
    ).reshape(per_rep, QH, 1)
    own_value = jnp.broadcast_to(own_value[:, :, None, :], (per_rep, KVH, 2, HD)).reshape(
        per_rep, QH, HD
    )
    new_top = jnp.maximum(top, own_score)
    keep = jnp.exp(top - new_top)
    own_weight = jnp.exp(own_score - new_top)
    mixed = (weighted * keep + own_weight * own_value) / (total * keep + own_weight)
    return mixed.reshape(per_rep, QH * HD).astype(BF16)


def layer(pre_query, pre_pairs, prefill_len, dec_query, dec_own, cache, cached_len, move):
    me = lax.axis_index("ctx").astype(jnp.int32)
    table = jnp.stack([me, prefill_len[0]]).astype(jnp.int32)
    pairs, query = pre_pairs[0], pre_query[0]
    key_1, value_1 = prefill_pairs(me, pre_pairs)
    dest_rep, lengths, source_rep = decode_tables(cache, cached_len, move)
    outgoing = after(decode_send(source_rep, dec_query), key_1, value_1)
    key_1, value_1 = swap(key_1, 2), swap(value_1, 6)
    arrived = exchange(outgoing)
    key_2, value_2 = prefill_pairs_on(me, pre_pairs, key_1, value_1)
    query_later = after(query, outgoing, key_2, value_2)
    key_2, value_2 = swap(key_2, 6), swap(value_2, 2)
    query_b1, query_x, query_a1 = prefill_queries(me, query_later)
    arrived = after(arrived, query_a1)
    query_a1, query_b1 = swap(query_a1, 2), swap(query_b1, 6)
    partial = decode_home(me, lengths, dest_rep, arrived, cache)
    back = exchange(partial)
    pairs_x = prefill_across(table, pairs, key_1, key_2, value_1, value_2)
    keyed = [pairs, key_1, key_2, value_1, value_2, pairs_x]
    query_a2 = swap(jnp.stack([wide(query, me ^ 6), query_a1[1]]), 6)
    query_b2 = swap(jnp.stack([query_x[1], query_b1[1]]), 2)
    back = decode_order(source_rep, back)
    other = swap(back, 1)
    out_5, out_4, out_32, token = part(
        table,
        keyed,
        [query_a1, query_a2, query_b2, back],
        [(8, 1, None), (7, 1, None), (8, 0, None), (6, 0, None)],
        [5, 4, 3, 2],
        [1, 1, 2],
    )
    back_5, back_4 = swap(out_5, 2), swap(out_4, 6)
    back_32 = swap(out_32, 2)
    back = packed(*merge(back, other))
    other = swap(back, 2)
    out_0, out_7, token = part(
        table,
        keyed,
        [query, query_b1, back, token],
        [(6, None, "query"), (7, 0, None)],
        [0, 7],
        [1, 1],
    )
    back_5 = swap(back_5, 6)
    back_4 = swap(back_4, 2)
    back_7 = swap(out_7, 6)
    back = packed(*merge(back, other))
    other = swap(back, 6)
    out_1, out_6, token = part(
        table, keyed, [query_a2, query_x, back, token], [(7, 0, None), (6, 0, None)], [1, 6], [1, 1]
    )
    back_6 = swap(out_6, 6)
    back_x = swap(jnp.concatenate([out_1, back_32[0:1], back_7, back_5]), 1)
    pre_out = prefill_join(table, [out_0, back_32, back_6, back_4, back_x])
    weighted, top, total = merge(back, other)
    dec_out = decode_finish(weighted, top, total, dec_query, dec_own)
    return (pre_out, dec_out)


def solution(mesh):
    in_specs = (
        P("rep", "ctx", None),
        P("rep", None, "ctx", None),
        P("rep"),
        P("rep", None),
        P("rep", None, None),
        P("rep", None, "ctx", None),
        P(),
        P(),
    )
    out_specs = (P("rep", "ctx", None), P("rep", None))
    return jax.shard_map(layer, mesh=mesh, in_specs=in_specs, out_specs=out_specs, check_vma=False)
```

```python
import functools
import math

import jax
import jax.numpy as jnp
from jax import lax
from jax.experimental import pallas as pl
from jax.experimental.pallas import tpu as pltpu
from jax.sharding import PartitionSpec as P


QH = 16
KVH = 8
HD = 128
SCALE = 1.0 / 12.0
EXP2_SCALE = SCALE * math.log2(math.e)
MASKED = -1e30
TILE = 128
CHUNK = 1024
VMEM = 54_000_000
SMALL = 20_000_000
BF16 = jnp.bfloat16
F32 = jnp.float32


def swap(array, flip):
    return lax.ppermute(array, "ctx", [(i, i ^ flip) for i in range(8)])


def exchange(array):
    return lax.all_to_all(array, "rep", split_axis=0, concat_axis=0, tiled=True)


def attend_kernel(table, *refs, key_pieces, value_pieces, query_pieces, blocks, out_sizes, count_in):
    inputs = refs[:count_in]
    out_refs = refs[count_in : count_in + len(out_sizes)]
    token = refs[count_in + len(out_sizes)]
    keys, values, queries, mixes, acc, top, sems, out_sems = refs[count_in + len(out_sizes) + 1 :]
    me = table[0]
    valid = table[1]
    core = me & 1
    copies = []

    def view(piece):
        which, index, kind = piece
        ref = inputs[which]
        if index is not None:
            ref = ref.at[index]
        if kind == "own":
            ref = ref.at[:, pl.ds(pl.multiple_of(me * HD, HD), HD)]
        elif kind == "core":
            ref = ref.at[:, pl.ds(pl.multiple_of(core * HD, HD), HD)]
        elif kind == "query":
            ref = ref.at[:, pl.ds(pl.multiple_of(me * 2 * HD, 2 * HD), 2 * HD)]
        return ref

    def put(piece, dest):
        copy = pltpu.make_async_copy(view(piece), dest, sems.at[len(copies)])
        copy.start()
        copies.append(copy)

    for z, piece in enumerate(key_pieces):
        at = pl.multiple_of((me ^ z) * 512, 512)
        put(piece, keys.at[pl.ds(at, 512)])
    for z, piece in enumerate(value_pieces):
        at = pl.multiple_of((me ^ z) * 512, 512)
        put(piece, values.at[pl.ds(at, 512), 0:HD])
    for n, piece in enumerate(query_pieces):
        put(piece, queries.at[n])
    values[:, HD:] = jnp.ones((values.shape[0], HD), BF16)
    for copy in copies:
        copy.wait()

    halves = 1
    parts = [(t, slice(t * TILE, (t + 1) * TILE)) for t in range(512 // TILE)]

    def one_block(n, block):
        first = block * 512

        @pl.when(first >= valid)
        def _():
            mixes[n] = jnp.zeros((512, 2 * HD), BF16)

        @pl.when(first < valid)
        def _():
            rest = first % CHUNK
            base = pl.multiple_of(first - rest, CHUNK)

            for start in range(0, CHUNK, 512):

                @pl.when(rest == start)
                def _(start=start):
                    for t, rows in parts:
                        width = start + (t + 1) * TILE
                        key = keys[pl.ds(base, width)]
                        value = values[pl.ds(base, width)]
                        seen = lax.broadcasted_iota(
                            jnp.int32, (TILE, width), 1
                        ) <= lax.broadcasted_iota(jnp.int32, (TILE, width), 0) + (width - TILE)
                        for g in range(2):
                            query = queries[n, rows, g * HD : (g + 1) * HD]
                            score = lax.dot_general(
                                query, key, (((1,), (1,)), ((), ())), preferred_element_type=F32
                            )
                            score = jnp.where(seen, score, MASKED)
                            new_top = jnp.max(score, axis=1, keepdims=True)
                            top[g, rows] = jnp.broadcast_to(new_top, (TILE, HD))
                            weight = jnp.exp2((score - new_top) * EXP2_SCALE).astype(BF16)
                            acc[g, rows] = jnp.dot(weight, value, preferred_element_type=F32)

            def full(at, chunk, rows_at, count):
                key = keys[pl.ds(at, chunk)]
                value = values[pl.ds(at, chunk)]
                for t in range(count):
                    rows = pl.ds(pl.multiple_of(rows_at + t * TILE, TILE), TILE)
                    for g in range(2):
                        query = queries[n, rows, g * HD : (g + 1) * HD]
                        score = lax.dot_general(
                            query, key, (((1,), (1,)), ((), ())), preferred_element_type=F32
                        )
                        old_top = top[g, rows]
                        new_top = jnp.maximum(old_top, jnp.max(score, axis=1, keepdims=True))
                        factor = jnp.exp2((old_top - new_top) * EXP2_SCALE)
                        top[g, rows] = new_top
                        weight = jnp.exp2((score - new_top[:, :1]) * EXP2_SCALE).astype(BF16)
                        more = jnp.dot(weight, value, preferred_element_type=F32)
                        acc[g, rows, :HD] = acc[g, rows, :HD] * factor + more[:, :HD]
                        acc[g, rows, HD:] = acc[g, rows, HD:] * factor + more[:, HD:]

            chunks = first // CHUNK

            def single(step, unused):
                at = pl.multiple_of((chunks - 1) * CHUNK, CHUNK)
                full(at, CHUNK, step * (512 // halves), 512 // TILE // halves)
                return unused

            def double(step, unused):
                full(pl.multiple_of(step * 2 * CHUNK, 2 * CHUNK), 2 * CHUNK, 0, 512 // TILE)
                return unused

            lax.fori_loop(0, (chunks % 2) * halves, single, 0)
            lax.fori_loop(0, chunks // 2, double, 0)
            live = lax.broadcasted_iota(jnp.int32, (512, HD), 0) + first < valid
            for g in range(2):
                mixed = acc[g, :, :HD] / acc[g, :, HD:]
                mixes[n, :, g * HD : (g + 1) * HD] = jnp.where(live, mixed, 0.0).astype(BF16)

    leaving = []
    for out_ref, size in zip(out_refs, out_sizes):
        for i in range(size):
            n = len(leaving)
            leaving.append(
                pltpu.make_async_copy(mixes.at[n], out_ref.at[i], out_sems.at[n])
            )

    def step(n, unused):
        flip = jnp.int32(blocks[0])
        for more in range(1, len(blocks)):
            flip = jnp.where(n == more, blocks[more], flip)
        one_block(n, me ^ flip)
        for at, copy in enumerate(leaving):

            @pl.when(n == at)
            def _(copy=copy):
                copy.start()

        return unused

    lax.fori_loop(0, len(blocks), step, 0)
    for copy in leaving:
        copy.wait()
    token[...] = jnp.zeros_like(token)


def attend_call(table, arrays, key_pieces, value_pieces, query_pieces, blocks, out_sizes):
    n = len(query_pieces)
    kernel = functools.partial(
        attend_kernel,
        key_pieces=key_pieces,
        value_pieces=value_pieces,
        query_pieces=query_pieces,
        blocks=blocks,
        out_sizes=out_sizes,
        count_in=len(arrays),
    )
    return pl.pallas_call(
        kernel,
        grid_spec=pltpu.PrefetchScalarGridSpec(
            num_scalar_prefetch=1,
            grid=(1,),
            in_specs=[pl.BlockSpec(memory_space=pl.ANY)] * len(arrays),
            out_specs=[pl.BlockSpec(memory_space=pl.ANY)] * len(out_sizes)
            + [pl.BlockSpec((8, HD), lambda i, t: (0, 0))],
            scratch_shapes=[
                pltpu.VMEM((4096, HD), BF16),
                pltpu.VMEM((4096, 2 * HD), BF16),
                pltpu.VMEM((n, 512, 2 * HD), BF16),
                pltpu.VMEM((n, 512, 2 * HD), BF16),
                pltpu.VMEM((2, 512, 2 * HD), F32),
                pltpu.VMEM((2, 512, HD), F32),
                pltpu.SemaphoreType.DMA((16 + n,)),
                pltpu.SemaphoreType.DMA((n,)),
            ],
        ),
        out_shape=[jax.ShapeDtypeStruct((size, 512, 2 * HD), BF16) for size in out_sizes]
        + [jax.ShapeDtypeStruct((8, HD), F32)],
        compiler_params=pltpu.CompilerParams(vmem_limit_bytes=SMALL),
        cost_estimate=pl.CostEstimate(
            flops=n * 1_200_000_000, bytes_accessed=4_000_000, transcendentals=n * 2_000_000
        ),
    )(table, *arrays)


def collect_kernel(table, *refs, outs, count_in):
    inputs = refs[:count_in]
    out_refs = refs[count_in:-1]
    sems = refs[-1]
    me = table[0]
    copies = []
    for out_ref, pieces in zip(out_refs, outs):
        for n, (which, index, lane, out_lane, width) in enumerate(pieces):
            ref = inputs[which]
            if index is not None:
                ref = ref.at[index]
            if lane is not None:
                ref = ref.at[:, pl.ds(pl.multiple_of(lane(me) * width, width), width)]
            if out_lane is None:
                dest = out_ref.at[n]
            else:
                at = pl.multiple_of(out_lane(me) * width, width)
                dest = out_ref.at[0, :, pl.ds(at, width)]
            copy = pltpu.make_async_copy(ref, dest, sems.at[len(copies)])
            copy.start()
            copies.append(copy)
    for copy in copies:
        copy.wait()


def collect(table, arrays, outs):
    shapes = []
    for pieces in outs:
        if pieces[0][3] is None:
            shapes.append((len(pieces), 512, pieces[0][4]))
        else:
            shapes.append((1, 512, len(pieces) * pieces[0][4]))
    total = sum(math.prod(shape) for shape in shapes)
    result = pl.pallas_call(
        functools.partial(collect_kernel, outs=outs, count_in=len(arrays)),
        grid_spec=pltpu.PrefetchScalarGridSpec(
            num_scalar_prefetch=1,
            grid=(1,),
            in_specs=[pl.BlockSpec(memory_space=pl.ANY)] * len(arrays),
            out_specs=[pl.BlockSpec(shape, lambda i, t: (0, 0, 0)) for shape in shapes],
            scratch_shapes=[pltpu.SemaphoreType.DMA((sum(len(p) for p in outs),))],
        ),
        out_shape=[jax.ShapeDtypeStruct(shape, BF16) for shape in shapes],
        compiler_params=pltpu.CompilerParams(vmem_limit_bytes=SMALL),
        cost_estimate=pl.CostEstimate(
            flops=total * 2, bytes_accessed=total * 4, transcendentals=0
        ),
    )(table, *arrays)
    return result


def after(value, *others):
    return lax.optimization_barrier((value, *others))[0]


def wide(query, at):
    return lax.dynamic_slice(query, (0, 0, at * 2 * HD), (1, 512, 2 * HD))


def wide_pairs(pairs, index, at):
    return lax.dynamic_slice(pairs, (0, index, 0, at * 2 * HD), (1, 1, 512, 2 * HD))[0]


def prefill_pairs(me, pairs):
    chip = me >> 1
    key_1 = jnp.concatenate([wide_pairs(pairs, 0, chip ^ 1), wide_pairs(pairs, 0, chip ^ 2)])
    value_1 = jnp.concatenate([wide_pairs(pairs, 1, chip ^ 3), wide_pairs(pairs, 1, chip ^ 2)])
    return key_1, value_1


def prefill_pairs_on(me, pairs, key_1, value_1):
    chip = me >> 1
    key_2 = jnp.concatenate([wide_pairs(pairs, 0, chip ^ 3), key_1[1:2]])
    value_2 = jnp.concatenate([wide_pairs(pairs, 1, chip ^ 1), value_1[1:2]])
    return key_2, value_2


def prefill_queries(me, query):
    query_x = swap(jnp.concatenate([wide(query, me ^ 7), wide(query, me ^ 5)]), 1)
    query_a1 = jnp.concatenate([wide(query, me ^ 2), wide(query, me ^ 4)])
    return query_x, query_a1


def prefill_across(table, pairs, key_1, key_2, value_1, value_2):
    def other(which, index):
        return (which, index, lambda m: 1 - (m & 1), None, HD)

    def own(index):
        return (0, index, lambda m: m ^ 1, None, HD)

    (pairs_x,) = collect(
        table,
        [pairs, key_1, key_2, value_1, value_2],
        [
            [
                own(0),
                other(1, 0),
                other(2, 1),
                other(2, 0),
                own(1),
                other(4, 0),
                other(4, 1),
                other(3, 0),
            ]
        ],
    )
    return swap(pairs_x, 1)


KEY_PIECES = [
    (0, 0, "own"),
    (5, 0, None),
    (1, 0, "core"),
    (5, 1, None),
    (2, 1, "core"),
    (5, 2, None),
    (2, 0, "core"),
    (5, 3, None),
]
VALUE_PIECES = [
    (0, 1, "own"),
    (5, 4, None),
    (4, 0, "core"),
    (5, 5, None),
    (4, 1, "core"),
    (5, 6, None),
    (3, 0, "core"),
    (5, 7, None),
]


def part(table, keyed, arrays, pieces, blocks, out_sizes):
    return attend_call(table, keyed + arrays, KEY_PIECES, VALUE_PIECES, pieces, blocks, out_sizes)


def prefill_join(table, outs):
    def place(which, index, z):
        return (which, index, None, lambda m: m ^ z, 2 * HD)

    places = [(0, 0), (4, 0), (1, 1), (4, 1), (3, 0), (4, 3), (2, 0), (4, 2)]
    (joined,) = collect(
        table, outs, [[place(which, index, z) for z, (which, index) in enumerate(places)]]
    )
    return joined


def cache_kernel(table, query_ref, cache_ref, out_ref):
    span_base = table[0]
    count = query_ref.shape[0]
    step_count, span = cache_ref.shape[0], cache_ref.shape[2]
    head = lax.broadcasted_iota(jnp.int32, (QH, KVH * HD), 0) // 2
    block = lax.broadcasted_iota(jnp.int32, (QH, KVH * HD), 1) // HD
    lane = lax.broadcasted_iota(jnp.int32, (QH, HD), 1)
    position = lax.broadcasted_iota(jnp.int32, (QH, span), 1) + span_base
    rows, scores, seen = [], [], []
    for i in range(step_count):
        n = pl.program_id(0) * step_count + i
        rows.append(table[1 + count + n])
        query = query_ref[rows[i]]
        wide = jnp.where(head == block, jnp.concatenate([query] * KVH, axis=1), 0).astype(BF16)
        scores.append(
            lax.dot_general(
                wide, cache_ref[i, 0], (((1,), (1,)), ((), ())), preferred_element_type=F32
            )
        )
        seen.append(position < table[1 + n])
    visible = jnp.concatenate(seen, axis=0)
    score = jnp.where(visible, jnp.concatenate(scores, axis=0) * SCALE, MASKED)
    top = jnp.max(score, axis=1, keepdims=True).astype(BF16).astype(F32)
    weight = jnp.where(visible, jnp.exp(score - top), 0.0)
    total = jnp.sum(weight, axis=1, keepdims=True)
    weight = weight.astype(BF16)
    for i in range(step_count):
        part = slice(i * QH, (i + 1) * QH)
        mixed = jnp.dot(weight[part], cache_ref[i, 1], preferred_element_type=F32)
        mixed = jnp.where(head == block, mixed, 0.0)
        picked = mixed[:, :HD]
        for h in range(1, KVH):
            picked = picked + mixed[:, h * HD : (h + 1) * HD]
        out_ref[rows[i], :, :HD] = picked.astype(BF16)
        out_ref[rows[i], :, HD:] = jnp.where(
            lane == 0,
            jnp.broadcast_to(top[part], (QH, HD)),
            jnp.broadcast_to(total[part], (QH, HD)),
        ).astype(BF16)


def over_cache(span_base, lengths, dest_rep, queries, cache):
    count = cache.shape[0]
    span = cache.shape[2]
    each = math.gcd(count, 4)
    table = jnp.concatenate([jnp.stack([span_base]), lengths, dest_rep]).astype(jnp.int32)
    return pl.pallas_call(
        cache_kernel,
        grid_spec=pltpu.PrefetchScalarGridSpec(
            num_scalar_prefetch=1,
            grid=(count // each,),
            in_specs=[
                pl.BlockSpec((count, QH, HD), lambda n, t: (0, 0, 0)),
                pl.BlockSpec((each, 2, span, KVH * HD), lambda n, t: (n, 0, 0, 0)),
            ],
            out_specs=pl.BlockSpec((count, QH, 2 * HD), lambda n, t: (0, 0, 0)),
        ),
        out_shape=jax.ShapeDtypeStruct((count, QH, 2 * HD), BF16),
        compiler_params=pltpu.CompilerParams(vmem_limit_bytes=VMEM),
        cost_estimate=pl.CostEstimate(
            flops=8_000_000_000, bytes_accessed=8_500_000, transcendentals=300_000
        ),
        name="over_cache",
    )(table, queries, cache)


def merge(left, right):
    left, right = left.astype(F32), right.astype(F32)
    left_top, right_top = left[..., HD : HD + 1], right[..., HD : HD + 1]
    new_top = jnp.maximum(left_top, right_top)
    left_factor = jnp.exp(left_top - new_top)
    right_factor = jnp.exp(right_top - new_top)
    weighted = left[..., :HD] * left_factor + right[..., :HD] * right_factor
    total = left[..., HD + 1 : HD + 2] * left_factor + right[..., HD + 1 : HD + 2] * right_factor
    return weighted, new_top, total


def packed(weighted, top, total):
    return jnp.concatenate([weighted, top, total], axis=-1).astype(BF16)


def decode_tables(cache, cached_len, move):
    per_rep = cache.shape[0]
    rep = lax.axis_index("rep")
    requests = move.shape[0]
    ids = jnp.arange(per_rep, dtype=jnp.int32)
    dest_rep = lax.dynamic_slice_in_dim(move, rep * per_rep, per_rep) // per_rep
    lengths = lax.dynamic_slice_in_dim(cached_len, rep * per_rep, per_rep)
    my_slots = rep * per_rep + ids
    served = jnp.sum(
        jnp.where(
            move[None, :] == my_slots[:, None], jnp.arange(requests, dtype=jnp.int32)[None, :], 0
        ),
        axis=1,
    )
    return dest_rep, lengths, served // per_rep


def decode_send(source_rep, dec_query):
    reps = lax.axis_size("rep")
    to_home = jnp.arange(reps, dtype=jnp.int32)[:, None] == source_rep[None, :]
    return jnp.dot(to_home.astype(BF16), dec_query, preferred_element_type=F32).astype(BF16)


def decode_home(me, lengths, dest_rep, arrived, cache):
    reps = lax.axis_size("rep")
    span = cache.shape[2]
    partial = over_cache(me * span, lengths, dest_rep, arrived.reshape(reps, QH, HD), cache)
    return partial[:, :, : HD + 2].reshape(reps, QH * (HD + 2))


def decode_order(source_rep, back):
    reps = back.shape[0]
    back = jnp.dot(
        (source_rep[:, None] == jnp.arange(reps, dtype=jnp.int32)[None, :]).astype(BF16),
        back,
        preferred_element_type=F32,
    ).astype(BF16)
    return back.reshape(source_rep.shape[0], QH, HD + 2)


def decode_finish(weighted, top, total, dec_query, dec_own):
    per_rep = dec_query.shape[0]
    query_heads = dec_query.reshape(per_rep, KVH, 2, HD)
    own_key = dec_own[:, 0].reshape(per_rep, KVH, HD)
    own_value = dec_own[:, 1].reshape(per_rep, KVH, HD).astype(F32)
    own_score = (
        jnp.sum(query_heads.astype(F32) * own_key[:, :, None, :].astype(F32), axis=-1) * SCALE
    ).reshape(per_rep, QH, 1)
    own_value = jnp.broadcast_to(own_value[:, :, None, :], (per_rep, KVH, 2, HD)).reshape(
        per_rep, QH, HD
    )
    new_top = jnp.maximum(top, own_score)
    keep = jnp.exp(top - new_top)
    own_weight = jnp.exp(own_score - new_top)
    mixed = (weighted * keep + own_weight * own_value) / (total * keep + own_weight)
    return mixed.reshape(per_rep, QH * HD).astype(BF16)


def layer(pre_query, pre_pairs, prefill_len, dec_query, dec_own, cache, cached_len, move):
    me = lax.axis_index("ctx").astype(jnp.int32)
    table = jnp.stack([me, prefill_len[0]]).astype(jnp.int32)
    pairs, query = pre_pairs[0], pre_query[0]
    key_1, value_1 = prefill_pairs(me, pre_pairs)
    query_later = after(pre_query, key_1, value_1)
    key_1, value_1 = swap(key_1, 2), swap(value_1, 6)
    query_b1, query_a1 = prefill_queries(me, query_later)
    dest_rep, lengths, source_rep = decode_tables(cache, cached_len, move)
    outgoing = after(decode_send(source_rep, dec_query), query_a1)
    query_a1, query_b1 = swap(query_a1, 2), swap(query_b1, 6)
    arrived = exchange(outgoing)
    key_2, value_2 = prefill_pairs_on(me, pre_pairs, key_1, value_1)
    query_later = after(pre_query, outgoing, key_2, value_2)
    key_2, value_2 = swap(key_2, 6), swap(value_2, 2)
    query_x = jnp.concatenate([wide(query_later, me ^ 1), wide(query_later, me ^ 3)])
    arrived = after(arrived, query_x)
    query_x = swap(query_x, 1)
    partial = decode_home(me, lengths, dest_rep, arrived, cache)
    back = exchange(partial)
    pairs_x = prefill_across(table, pairs, key_1, key_2, value_1, value_2)
    keyed = [pairs, key_1, key_2, value_1, value_2, pairs_x]
    query_a2 = swap(jnp.concatenate([wide(pre_query, me ^ 6), query_a1[1:2]]), 6)
    query_b2 = swap(jnp.concatenate([query_x[1:2], query_b1[1:2]]), 2)
    out_5, out_4, out_32, token = part(
        table,
        keyed,
        [query_a1, query_a2, query_b2, partial],
        [(8, 1, None), (7, 1, None), (8, 0, None), (6, 0, None)],
        [5, 4, 3, 2],
        [1, 1, 2],
    )
    back_5, back_4 = swap(out_5, 2), swap(out_4, 6)
    back_32 = swap(out_32, 2)
    back = decode_order(source_rep, after(back, token))
    other = swap(back, 6)
    out_0, out_7, token = part(
        table,
        keyed,
        [query, query_b1, back, token],
        [(6, None, "query"), (7, 0, None)],
        [0, 7],
        [1, 1],
    )
    back_5 = swap(back_5, 6)
    back_4 = swap(back_4, 2)
    back_7 = swap(out_7, 6)
    back = packed(*merge(back, other))
    other = swap(back, 2)
    out_1, out_6, token = part(
        table, keyed, [query_a2, query_x, back, token], [(7, 0, None), (6, 0, None)], [1, 6], [1, 1]
    )
    back_6 = swap(out_6, 6)
    back = packed(*merge(back, after(other, token)))
    other = swap(back, 1)
    back_x = swap(jnp.concatenate([out_1, back_32[0:1], back_7, back_5]), 1)
    pre_out = prefill_join(table, [out_0, back_32, back_6, back_4, back_x])
    weighted, top, total = merge(back, other)
    dec_out = decode_finish(weighted, top, total, dec_query, dec_own)
    return (pre_out, dec_out)


def solution(mesh):
    in_specs = (
        P("rep", "ctx", None),
        P("rep", None, "ctx", None),
        P("rep"),
        P("rep", None),
        P("rep", None, None),
        P("rep", None, "ctx", None),
        P(),
        P(),
    )
    out_specs = (P("rep", "ctx", None), P("rep", None))
    return jax.shard_map(layer, mesh=mesh, in_specs=in_specs, out_specs=out_specs, check_vma=False)
```

```python
import functools
import math

import jax
import jax.numpy as jnp
from jax import lax
from jax.experimental import pallas as pl
from jax.experimental.pallas import tpu as pltpu
from jax.sharding import PartitionSpec as P


QH = 16
KVH = 8
HD = 128
SCALE = 1.0 / 12.0
EXP2_SCALE = SCALE * math.log2(math.e)
MASKED = -1e30
TILE = 128
CHUNK = 1024
VMEM = 54_000_000
SMALL = 20_000_000
BF16 = jnp.bfloat16
F32 = jnp.float32


def swap(array, flip):
    return lax.ppermute(array, "ctx", [(i, i ^ flip) for i in range(8)])


def exchange(array):
    return lax.all_to_all(array, "rep", split_axis=0, concat_axis=0, tiled=True)


def attend_kernel(table, *refs, key_pieces, value_pieces, query_pieces, blocks, out_sizes, count_in):
    inputs = refs[:count_in]
    out_refs = refs[count_in : count_in + len(out_sizes)]
    token = refs[count_in + len(out_sizes)]
    keys, values, queries, mixes, acc, top, sems, out_sems = refs[count_in + len(out_sizes) + 1 :]
    me = table[0]
    valid = table[1]
    core = me & 1
    copies = []

    def view(piece):
        which, index, kind = piece
        ref = inputs[which]
        if index is not None:
            ref = ref.at[index]
        if kind == "own":
            ref = ref.at[:, pl.ds(pl.multiple_of(me * HD, HD), HD)]
        elif kind == "core":
            ref = ref.at[:, pl.ds(pl.multiple_of(core * HD, HD), HD)]
        elif kind == "query":
            ref = ref.at[:, pl.ds(pl.multiple_of(me * 2 * HD, 2 * HD), 2 * HD)]
        return ref

    def put(piece, dest):
        copy = pltpu.make_async_copy(view(piece), dest, sems.at[len(copies)])
        copy.start()
        copies.append(copy)

    for z, piece in enumerate(key_pieces):
        at = pl.multiple_of((me ^ z) * 512, 512)
        put(piece, keys.at[pl.ds(at, 512)])
    for z, piece in enumerate(value_pieces):
        at = pl.multiple_of((me ^ z) * 512, 512)
        put(piece, values.at[pl.ds(at, 512), 0:HD])
    for n, piece in enumerate(query_pieces):
        put(piece, queries.at[n])
    values[:, HD:] = jnp.ones((values.shape[0], HD), BF16)
    for copy in copies:
        copy.wait()

    halves = 1
    parts = [(t, slice(t * TILE, (t + 1) * TILE)) for t in range(512 // TILE)]

    def one_block(n, block):
        first = block * 512

        @pl.when(first >= valid)
        def _():
            mixes[n] = jnp.zeros((512, 2 * HD), BF16)

        @pl.when(first < valid)
        def _():
            rest = first % CHUNK
            base = pl.multiple_of(first - rest, CHUNK)

            for start in range(0, CHUNK, 512):

                @pl.when(rest == start)
                def _(start=start):
                    for t, rows in parts:
                        width = start + (t + 1) * TILE
                        key = keys[pl.ds(base, width)]
                        value = values[pl.ds(base, width)]
                        seen = lax.broadcasted_iota(
                            jnp.int32, (TILE, width), 1
                        ) <= lax.broadcasted_iota(jnp.int32, (TILE, width), 0) + (width - TILE)
                        for g in range(2):
                            query = queries[n, rows, g * HD : (g + 1) * HD]
                            score = lax.dot_general(
                                query, key, (((1,), (1,)), ((), ())), preferred_element_type=F32
                            )
                            score = jnp.where(seen, score, MASKED)
                            new_top = jnp.max(score, axis=1, keepdims=True)
                            top[g, rows] = jnp.broadcast_to(new_top, (TILE, HD))
                            weight = jnp.exp2((score - new_top) * EXP2_SCALE).astype(BF16)
                            acc[g, rows] = jnp.dot(weight, value, preferred_element_type=F32)

            def full(at, chunk, rows_at, count):
                key = keys[pl.ds(at, chunk)]
                value = values[pl.ds(at, chunk)]
                for t in range(count):
                    rows = pl.ds(pl.multiple_of(rows_at + t * TILE, TILE), TILE)
                    for g in range(2):
                        query = queries[n, rows, g * HD : (g + 1) * HD]
                        score = lax.dot_general(
                            query, key, (((1,), (1,)), ((), ())), preferred_element_type=F32
                        )
                        old_top = top[g, rows]
                        new_top = jnp.maximum(old_top, jnp.max(score, axis=1, keepdims=True))
                        factor = jnp.exp2((old_top - new_top) * EXP2_SCALE)
                        top[g, rows] = new_top
                        weight = jnp.exp2((score - new_top[:, :1]) * EXP2_SCALE).astype(BF16)
                        more = jnp.dot(weight, value, preferred_element_type=F32)
                        acc[g, rows, :HD] = acc[g, rows, :HD] * factor + more[:, :HD]
                        acc[g, rows, HD:] = acc[g, rows, HD:] * factor + more[:, HD:]

            chunks = first // CHUNK

            def single(step, unused):
                at = pl.multiple_of((chunks - 1) * CHUNK, CHUNK)
                full(at, CHUNK, step * (512 // halves), 512 // TILE // halves)
                return unused

            def double(step, unused):
                full(pl.multiple_of(step * 2 * CHUNK, 2 * CHUNK), 2 * CHUNK, 0, 512 // TILE)
                return unused

            lax.fori_loop(0, (chunks % 2) * halves, single, 0)
            lax.fori_loop(0, chunks // 2, double, 0)
            live = lax.broadcasted_iota(jnp.int32, (512, HD), 0) + first < valid
            for g in range(2):
                mixed = acc[g, :, :HD] / acc[g, :, HD:]
                mixes[n, :, g * HD : (g + 1) * HD] = jnp.where(live, mixed, 0.0).astype(BF16)

    leaving = []
    for out_ref, size in zip(out_refs, out_sizes):
        for i in range(size):
            n = len(leaving)
            leaving.append(
                pltpu.make_async_copy(mixes.at[n], out_ref.at[i], out_sems.at[n])
            )

    def step(n, unused):
        flip = jnp.int32(blocks[0])
        for more in range(1, len(blocks)):
            flip = jnp.where(n == more, blocks[more], flip)
        one_block(n, me ^ flip)
        for at, copy in enumerate(leaving):

            @pl.when(n == at)
            def _(copy=copy):
                copy.start()

        return unused

    lax.fori_loop(0, len(blocks), step, 0)
    for copy in leaving:
        copy.wait()
    token[...] = jnp.zeros_like(token)


def attend_call(table, arrays, key_pieces, value_pieces, query_pieces, blocks, out_sizes):
    n = len(query_pieces)
    kernel = functools.partial(
        attend_kernel,
        key_pieces=key_pieces,
        value_pieces=value_pieces,
        query_pieces=query_pieces,
        blocks=blocks,
        out_sizes=out_sizes,
        count_in=len(arrays),
    )
    return pl.pallas_call(
        kernel,
        grid_spec=pltpu.PrefetchScalarGridSpec(
            num_scalar_prefetch=1,
            grid=(1,),
            in_specs=[pl.BlockSpec(memory_space=pl.ANY)] * len(arrays),
            out_specs=[pl.BlockSpec(memory_space=pl.ANY)] * len(out_sizes)
            + [pl.BlockSpec((8, HD), lambda i, t: (0, 0))],
            scratch_shapes=[
                pltpu.VMEM((4096, HD), BF16),
                pltpu.VMEM((4096, 2 * HD), BF16),
                pltpu.VMEM((n, 512, 2 * HD), BF16),
                pltpu.VMEM((n, 512, 2 * HD), BF16),
                pltpu.VMEM((2, 512, 2 * HD), F32),
                pltpu.VMEM((2, 512, HD), F32),
                pltpu.SemaphoreType.DMA((16 + n,)),
                pltpu.SemaphoreType.DMA((n,)),
            ],
        ),
        out_shape=[jax.ShapeDtypeStruct((size, 512, 2 * HD), BF16) for size in out_sizes]
        + [jax.ShapeDtypeStruct((8, HD), F32)],
        compiler_params=pltpu.CompilerParams(vmem_limit_bytes=SMALL),
        cost_estimate=pl.CostEstimate(
            flops=n * 1_200_000_000, bytes_accessed=4_000_000, transcendentals=n * 2_000_000
        ),
    )(table, *arrays)


def collect_kernel(table, *refs, outs, count_in):
    inputs = refs[:count_in]
    out_refs = refs[count_in:-1]
    sems = refs[-1]
    me = table[0]
    copies = []
    for out_ref, pieces in zip(out_refs, outs):
        for n, (which, index, lane, out_lane, width) in enumerate(pieces):
            ref = inputs[which]
            if index is not None:
                ref = ref.at[index]
            if lane is not None:
                ref = ref.at[:, pl.ds(pl.multiple_of(lane(me) * width, width), width)]
            if out_lane is None:
                dest = out_ref.at[n]
            else:
                at = pl.multiple_of(out_lane(me) * width, width)
                dest = out_ref.at[0, :, pl.ds(at, width)]
            copy = pltpu.make_async_copy(ref, dest, sems.at[len(copies)])
            copy.start()
            copies.append(copy)
    for copy in copies:
        copy.wait()


def collect(table, arrays, outs):
    shapes = []
    for pieces in outs:
        if pieces[0][3] is None:
            shapes.append((len(pieces), 512, pieces[0][4]))
        else:
            shapes.append((1, 512, len(pieces) * pieces[0][4]))
    total = sum(math.prod(shape) for shape in shapes)
    result = pl.pallas_call(
        functools.partial(collect_kernel, outs=outs, count_in=len(arrays)),
        grid_spec=pltpu.PrefetchScalarGridSpec(
            num_scalar_prefetch=1,
            grid=(1,),
            in_specs=[pl.BlockSpec(memory_space=pl.ANY)] * len(arrays),
            out_specs=[pl.BlockSpec(shape, lambda i, t: (0, 0, 0)) for shape in shapes],
            scratch_shapes=[pltpu.SemaphoreType.DMA((sum(len(p) for p in outs),))],
        ),
        out_shape=[jax.ShapeDtypeStruct(shape, BF16) for shape in shapes],
        compiler_params=pltpu.CompilerParams(vmem_limit_bytes=SMALL),
        cost_estimate=pl.CostEstimate(
            flops=total * 2, bytes_accessed=total * 4, transcendentals=0
        ),
    )(table, *arrays)
    return result


def after(value, *others):
    return lax.optimization_barrier((value, *others))[0]


def wide(query, at):
    return lax.dynamic_slice(query, (0, 0, at * 2 * HD), (1, 512, 2 * HD))


def wide_pairs(pairs, index, at):
    return lax.dynamic_slice(pairs, (0, index, 0, at * 2 * HD), (1, 1, 512, 2 * HD))[0]


def prefill_pairs(me, pairs):
    chip = me >> 1
    key_1 = jnp.concatenate([wide_pairs(pairs, 0, chip ^ 1), wide_pairs(pairs, 0, chip ^ 2)])
    value_1 = jnp.concatenate([wide_pairs(pairs, 1, chip ^ 3), wide_pairs(pairs, 1, chip ^ 2)])
    return key_1, value_1


def prefill_pairs_on(me, pairs, key_1, value_1):
    chip = me >> 1
    key_2 = jnp.concatenate([wide_pairs(pairs, 0, chip ^ 3), key_1[1:2]])
    value_2 = jnp.concatenate([wide_pairs(pairs, 1, chip ^ 1), value_1[1:2]])
    return key_2, value_2


def prefill_queries(me, query):
    query_x = swap(jnp.concatenate([wide(query, me ^ 7), wide(query, me ^ 5)]), 1)
    query_a1 = jnp.concatenate([wide(query, me ^ 2), wide(query, me ^ 4)])
    return query_x, query_a1


def prefill_across(table, pairs, key_1, key_2, value_1, value_2):
    def other(which, index):
        return (which, index, lambda m: 1 - (m & 1), None, HD)

    def own(index):
        return (0, index, lambda m: m ^ 1, None, HD)

    (pairs_x,) = collect(
        table,
        [pairs, key_1, key_2, value_1, value_2],
        [
            [
                own(0),
                other(1, 0),
                other(2, 1),
                other(2, 0),
                own(1),
                other(4, 0),
                other(4, 1),
                other(3, 0),
            ]
        ],
    )
    return swap(pairs_x, 1)


KEY_PIECES = [
    (0, 0, "own"),
    (5, 0, None),
    (1, 0, "core"),
    (5, 1, None),
    (2, 1, "core"),
    (5, 2, None),
    (2, 0, "core"),
    (5, 3, None),
]
VALUE_PIECES = [
    (0, 1, "own"),
    (5, 4, None),
    (4, 0, "core"),
    (5, 5, None),
    (4, 1, "core"),
    (5, 6, None),
    (3, 0, "core"),
    (5, 7, None),
]


def part(table, keyed, arrays, pieces, blocks, out_sizes):
    return attend_call(table, keyed + arrays, KEY_PIECES, VALUE_PIECES, pieces, blocks, out_sizes)


def prefill_join(table, outs):
    def place(which, index, z):
        return (which, index, None, lambda m: m ^ z, 2 * HD)

    places = [(0, 0), (4, 0), (1, 1), (4, 1), (3, 0), (4, 3), (2, 0), (4, 2)]
    (joined,) = collect(
        table, outs, [[place(which, index, z) for z, (which, index) in enumerate(places)]]
    )
    return joined


def cache_kernel(table, query_ref, cache_ref, out_ref):
    span_base = table[0]
    count = query_ref.shape[0]
    step_count, span = cache_ref.shape[0], cache_ref.shape[2]
    head = lax.broadcasted_iota(jnp.int32, (QH, KVH * HD), 0) // 2
    block = lax.broadcasted_iota(jnp.int32, (QH, KVH * HD), 1) // HD
    lane = lax.broadcasted_iota(jnp.int32, (QH, HD), 1)
    position = lax.broadcasted_iota(jnp.int32, (QH, span), 1) + span_base
    rows, scores, seen = [], [], []
    for i in range(step_count):
        n = pl.program_id(0) * step_count + i
        rows.append(table[1 + count + n])
        query = query_ref[rows[i]]
        wide = jnp.where(head == block, jnp.concatenate([query] * KVH, axis=1), 0).astype(BF16)
        scores.append(
            lax.dot_general(
                wide, cache_ref[i, 0], (((1,), (1,)), ((), ())), preferred_element_type=F32
            )
        )
        seen.append(position < table[1 + n])
    visible = jnp.concatenate(seen, axis=0)
    score = jnp.where(visible, jnp.concatenate(scores, axis=0) * SCALE, MASKED)
    top = jnp.max(score, axis=1, keepdims=True).astype(BF16).astype(F32)
    weight = jnp.where(visible, jnp.exp(score - top), 0.0)
    total = jnp.sum(weight, axis=1, keepdims=True)
    weight = weight.astype(BF16)
    for i in range(step_count):
        part = slice(i * QH, (i + 1) * QH)
        mixed = jnp.dot(weight[part], cache_ref[i, 1], preferred_element_type=F32)
        mixed = jnp.where(head == block, mixed, 0.0)
        picked = mixed[:, :HD]
        for h in range(1, KVH):
            picked = picked + mixed[:, h * HD : (h + 1) * HD]
        out_ref[rows[i], :, :HD] = picked.astype(BF16)
        out_ref[rows[i], :, HD:] = jnp.where(
            lane == 0,
            jnp.broadcast_to(top[part], (QH, HD)),
            jnp.broadcast_to(total[part], (QH, HD)),
        ).astype(BF16)


def over_cache(span_base, lengths, dest_rep, queries, cache):
    count = cache.shape[0]
    span = cache.shape[2]
    each = math.gcd(count, 4)
    table = jnp.concatenate([jnp.stack([span_base]), lengths, dest_rep]).astype(jnp.int32)
    return pl.pallas_call(
        cache_kernel,
        grid_spec=pltpu.PrefetchScalarGridSpec(
            num_scalar_prefetch=1,
            grid=(count // each,),
            in_specs=[
                pl.BlockSpec((count, QH, HD), lambda n, t: (0, 0, 0)),
                pl.BlockSpec((each, 2, span, KVH * HD), lambda n, t: (n, 0, 0, 0)),
            ],
            out_specs=pl.BlockSpec((count, QH, 2 * HD), lambda n, t: (0, 0, 0)),
        ),
        out_shape=jax.ShapeDtypeStruct((count, QH, 2 * HD), BF16),
        compiler_params=pltpu.CompilerParams(vmem_limit_bytes=VMEM),
        cost_estimate=pl.CostEstimate(
            flops=8_000_000_000, bytes_accessed=8_500_000, transcendentals=300_000
        ),
        name="over_cache",
    )(table, queries, cache)


def merge(left, right):
    left, right = left.astype(F32), right.astype(F32)
    left_top, right_top = left[..., HD : HD + 1], right[..., HD : HD + 1]
    new_top = jnp.maximum(left_top, right_top)
    left_factor = jnp.exp(left_top - new_top)
    right_factor = jnp.exp(right_top - new_top)
    weighted = left[..., :HD] * left_factor + right[..., :HD] * right_factor
    total = left[..., HD + 1 : HD + 2] * left_factor + right[..., HD + 1 : HD + 2] * right_factor
    return weighted, new_top, total


def packed(weighted, top, total):
    return jnp.concatenate([weighted, top, total], axis=-1).astype(BF16)


def decode_tables(cache, cached_len, move):
    per_rep = cache.shape[0]
    rep = lax.axis_index("rep")
    requests = move.shape[0]
    ids = jnp.arange(per_rep, dtype=jnp.int32)
    dest_rep = lax.dynamic_slice_in_dim(move, rep * per_rep, per_rep) // per_rep
    lengths = lax.dynamic_slice_in_dim(cached_len, rep * per_rep, per_rep)
    my_slots = rep * per_rep + ids
    served = jnp.sum(
        jnp.where(
            move[None, :] == my_slots[:, None], jnp.arange(requests, dtype=jnp.int32)[None, :], 0
        ),
        axis=1,
    )
    return dest_rep, lengths, served // per_rep


def decode_send(source_rep, dec_query):
    reps = lax.axis_size("rep")
    to_home = jnp.arange(reps, dtype=jnp.int32)[:, None] == source_rep[None, :]
    return jnp.dot(to_home.astype(BF16), dec_query, preferred_element_type=F32).astype(BF16)


def decode_home(me, lengths, dest_rep, arrived, cache):
    reps = lax.axis_size("rep")
    span = cache.shape[2]
    partial = over_cache(me * span, lengths, dest_rep, arrived.reshape(reps, QH, HD), cache)
    return partial[:, :, : HD + 2].reshape(reps, QH * (HD + 2))


def decode_order(source_rep, back):
    reps = back.shape[0]
    back = jnp.dot(
        (source_rep[:, None] == jnp.arange(reps, dtype=jnp.int32)[None, :]).astype(BF16),
        back,
        preferred_element_type=F32,
    ).astype(BF16)
    return back.reshape(source_rep.shape[0], QH, HD + 2)


def decode_finish(weighted, top, total, dec_query, dec_own):
    per_rep = dec_query.shape[0]
    query_heads = dec_query.reshape(per_rep, KVH, 2, HD)
    own_key = dec_own[:, 0].reshape(per_rep, KVH, HD)
    own_value = dec_own[:, 1].reshape(per_rep, KVH, HD).astype(F32)
    own_score = (
        jnp.sum(query_heads.astype(F32) * own_key[:, :, None, :].astype(F32), axis=-1) * SCALE
    ).reshape(per_rep, QH, 1)
    own_value = jnp.broadcast_to(own_value[:, :, None, :], (per_rep, KVH, 2, HD)).reshape(
        per_rep, QH, HD
    )
    new_top = jnp.maximum(top, own_score)
    keep = jnp.exp(top - new_top)
    own_weight = jnp.exp(own_score - new_top)
    mixed = (weighted * keep + own_weight * own_value) / (total * keep + own_weight)
    return mixed.reshape(per_rep, QH * HD).astype(BF16)


def layer(pre_query, pre_pairs, prefill_len, dec_query, dec_own, cache, cached_len, move):
    me = lax.axis_index("ctx").astype(jnp.int32)
    table = jnp.stack([me, prefill_len[0]]).astype(jnp.int32)
    pairs, query = pre_pairs[0], pre_query[0]
    key_1, value_1 = prefill_pairs(me, pre_pairs)
    query_later = after(pre_query, key_1, value_1)
    key_1, value_1 = swap(key_1, 2), swap(value_1, 6)
    query_b1, query_a1 = prefill_queries(me, query_later)
    dest_rep, lengths, source_rep = decode_tables(cache, cached_len, move)
    outgoing = after(decode_send(source_rep, dec_query), query_a1)
    query_a1, query_b1 = swap(query_a1, 2), swap(query_b1, 6)
    arrived = exchange(outgoing)
    key_2, value_2 = prefill_pairs_on(me, pre_pairs, key_1, value_1)
    query_later = after(pre_query, outgoing, key_2, value_2)
    key_2, value_2 = swap(key_2, 6), swap(value_2, 2)
    query_x = jnp.concatenate([wide(query_later, me ^ 1), wide(query_later, me ^ 3)])
    arrived = after(arrived, query_x)
    query_x = swap(query_x, 1)
    partial = decode_home(me, lengths, dest_rep, arrived, cache)
    back = exchange(partial)
    pairs_x = prefill_across(table, pairs, key_1, key_2, value_1, value_2)
    keyed = [pairs, key_1, key_2, value_1, value_2, pairs_x]
    query_a2 = swap(jnp.concatenate([wide(pre_query, me ^ 6), query_a1[1:2]]), 6)
    query_b2 = swap(jnp.concatenate([query_x[1:2], query_b1[1:2]]), 2)
    out_5, out_4, out_32, token = part(
        table,
        keyed,
        [query_a1, query_a2, query_b2, partial],
        [(8, 1, None), (7, 1, None), (8, 0, None), (6, 0, None)],
        [5, 4, 3, 2],
        [1, 1, 2],
    )
    back_5, back_4 = swap(out_5, 2), swap(out_4, 6)
    back_32 = swap(out_32, 2)
    back = decode_order(source_rep, after(back, token))
    back = packed(*merge(back, swap(back, 1)))
    other = swap(back, 6)
    out_0, out_7, token = part(
        table,
        keyed,
        [query, query_b1, back, token],
        [(6, None, "query"), (7, 0, None)],
        [0, 7],
        [1, 1],
    )
    back_5 = swap(back_5, 6)
    back_4 = swap(back_4, 2)
    back_7 = swap(out_7, 6)
    back = packed(*merge(back, other))
    other = swap(back, 2)
    out_1, out_6, token = part(
        table, keyed, [query_a2, query_x, back, token], [(7, 0, None), (6, 0, None)], [1, 6], [1, 1]
    )
    back_6 = swap(out_6, 6)
    back_x = swap(jnp.concatenate([out_1, back_32[0:1], back_7, back_5]), 1)
    pre_out = prefill_join(table, [out_0, back_32, back_6, back_4, back_x])
    weighted, top, total = merge(back, after(other, token))
    dec_out = decode_finish(weighted, top, total, dec_query, dec_own)
    return (pre_out, dec_out)


def solution(mesh):
    in_specs = (
        P("rep", "ctx", None),
        P("rep", None, "ctx", None),
        P("rep"),
        P("rep", None),
        P("rep", None, None),
        P("rep", None, "ctx", None),
        P(),
        P(),
    )
    out_specs = (P("rep", "ctx", None), P("rep", None))
    return jax.shard_map(layer, mesh=mesh, in_specs=in_specs, out_specs=out_specs, check_vma=False)
```
